32 devices in a mesh: row: 4 (over y, core), col: 8 (over z, x).
Axes of the slice: x: 2, y: 2, z: 4, core: 2. Of those that a mesh axis runs over, the one named last changes fastest.
Arguments:
- tokens: bfloat16 [40, 8192], P('col', 'row'), may hold values from -6 to 6
- grad_out: bfloat16 [40, 8192], P('col', 'row'), may hold values from -6 to 6
- gate_weight: bfloat16 [8192, 28672], P('row', 'col'), may hold values from -0.0625 to 0.0625
- up_weight: bfloat16 [8192, 28672], P('row', 'col'), may hold values from -0.0625 to 0.0625
- down_weight: bfloat16 [28672, 8192], P('col', 'row'), may hold values from -0.03125 to 0.03125
Outputs:
- grad_tokens: bfloat16 [40, 8192], P('col', 'row')
- grad_gate_weight: bfloat16 [8192, 28672], P('row', 'col')
- grad_up_weight: bfloat16 [8192, 28672], P('row', 'col')
- grad_down_weight: bfloat16 [28672, 8192], P('col', 'row')
The draws below stay inside these ranges and needn't reach their ends.
All inputs are finite; a program needn't handle non-finite values.
Results may differ from the reference program's by a relative error of at most 0.0049.
Values may be sent and summed in bfloat16 or wider, within the bound.
No kernel may reach another device: no remote copies, remote signals or barrier semaphores. Data moves between devices by JAX's collectives and lax.ppermute only.
A program may use at most 192 MiB of HBM per device.

```python
import jax
import jax.numpy as jnp

D = 8192
FF = 28672
TOKENS = 40


def steps_of(stream_key, dims, shards, low, top_value):
    def one(axis_at, blocks):
        steps = jax.random.uniform(jax.random.fold_in(jax.random.fold_in(stream_key, 6), axis_at), (blocks,), jnp.float32, low / len(shards), top_value / len(shards))
        return jnp.repeat(jnp.exp(steps), dims[axis_at] // blocks).reshape((-1,) + (1,) * (len(dims) - axis_at - 1))

    factor_of = one(*shards[0])
    for cut in shards[1:]:
        factor_of = factor_of * one(*cut)
    return factor_of


def gaussian(key, shape, spread, reach, pieces=(), dtype=jnp.bfloat16):
    gain = steps_of(key, shape, pieces, -0.22, 0.18) if pieces else 1.0
    array = jax.random.normal(key, shape, jnp.float32) * spread * gain
    return jnp.minimum(jnp.maximum(array, -reach), reach).astype(dtype)


def setup_inputs(seed: int = 0) -> dict:
    seeds = jax.random.split(jax.random.key(seed), 6)
    tokens = gaussian(seeds[0], (TOKENS, D), 1.0, 6.0, ((0, 8), (1, 4)))
    grad_out = gaussian(seeds[1], (TOKENS, D), 1.0, 6.0, ((0, 8), (1, 4)))
    gate_weight = gaussian(seeds[2], (D, FF), D ** -0.5, 0.0625, ((0, 4), (1, 8)))
    up_weight = gaussian(seeds[3], (D, FF), D ** -0.5, 0.0625, ((0, 4), (1, 8)))
    down_weight = gaussian(seeds[4], (FF, D), FF ** -0.5, 0.03125, ((0, 8), (1, 4)))
    return dict(tokens=tokens, grad_out=grad_out, gate_weight=gate_weight, up_weight=up_weight, down_weight=down_weight)


def hidden_grads(gate_sum, up_sum, back_sum):
    sigmoid_gate = 1.0 / (1.0 + jnp.exp(-gate_sum))
    activated = gate_sum * sigmoid_gate
    hidden = (activated * up_sum).astype(jnp.bfloat16)
    grad_up = (back_sum * activated).astype(jnp.bfloat16)
    slope = sigmoid_gate * (1.0 + gate_sum * (1.0 - sigmoid_gate))
    grad_gate = (back_sum * up_sum * slope).astype(jnp.bfloat16)
    return hidden, grad_gate, grad_up


def reference(tokens, grad_out, gate_weight, up_weight, down_weight):
    gate_sum = jnp.dot(tokens, gate_weight, preferred_element_type=jnp.float32)
    up_sum = jnp.dot(tokens, up_weight, preferred_element_type=jnp.float32)
    back_sum = jnp.dot(grad_out, down_weight.T, preferred_element_type=jnp.float32)
    hidden, grad_gate, grad_up = hidden_grads(gate_sum, up_sum, back_sum)
    grad_down_weight = jnp.dot(hidden.T, grad_out, preferred_element_type=jnp.float32).astype(jnp.bfloat16)
    grad_gate_weight = jnp.dot(tokens.T, grad_gate, preferred_element_type=jnp.float32).astype(jnp.bfloat16)
    grad_up_weight = jnp.dot(tokens.T, grad_up, preferred_element_type=jnp.float32).astype(jnp.bfloat16)
    grad_tokens = jnp.dot(grad_gate, gate_weight.T, preferred_element_type=jnp.float32)
    grad_tokens = grad_tokens + jnp.dot(grad_up, up_weight.T, preferred_element_type=jnp.float32)
    return grad_tokens.astype(jnp.bfloat16), grad_gate_weight, grad_up_weight, grad_down_weight
```

```python
import jax
import jax.numpy as jnp
from jax import lax
from jax.experimental import pallas as pl
from jax.experimental.pallas import tpu as pltpu
from jax.sharding import PartitionSpec as P

BF = jnp.bfloat16
F32 = jnp.float32
NT = (((1,), (1,)), ((), ()))
TN = (((0,), (0,)), ((), ()))
VMEM = pl.BlockSpec(memory_space=pltpu.VMEM)


def block_of(size, unit, most):
    fits = [b for b in range(unit, min(size, most) + 1, unit) if size % b == 0]
    return fits[-1] if fits else size


def slab(i, size, whole):
    return slice(None) if size == whole else pl.ds(pl.multiple_of(i * size, size), size)


def params(limit, arbitrary=True):
    return pltpu.CompilerParams(
        vmem_limit_bytes=limit,
        dimension_semantics=("arbitrary",) if arbitrary else None,
    )


def load_body(*refs):
    n = len(refs) // 2
    sems = refs[-1]
    copies = [pltpu.make_async_copy(refs[i], refs[n + i], sems.at[i]) for i in range(n)]
    for copy in copies:
        copy.start()
    for copy in copies:
        copy.wait()


def load(*arrays):
    return pl.pallas_call(
        load_body,
        out_shape=tuple(pltpu.VMEM(a.shape, a.dtype) for a in arrays),
        in_specs=[pl.BlockSpec(memory_space=pltpu.HBM)] * len(arrays),
        out_specs=(VMEM,) * len(arrays),
        scratch_shapes=[pltpu.SemaphoreType.DMA((len(arrays),))],
        compiler_params=params(1 << 20, False),
        cost_estimate=pl.CostEstimate(
            flops=20_000_000_000, transcendentals=0, bytes_accessed=2 * sum(a.size * 2 for a in arrays)
        ),
        name="load",
    )(*arrays)


def dot(a, b, dims=(((1,), (0,)), ((), ()))):
    return lax.dot_general(a, b, dims, preferred_element_type=F32)


def sums_body(half, block, pick, pieces, gate_w, up_w, down_w, mine, send, tok, grad):
    j = pl.program_id(0)

    @pl.when(j == 0)
    def _():
        tok[...] = dot(pick[...], pieces[0]).astype(BF)
        grad[...] = dot(pick[...], pieces[1]).astype(BF)

    cols = slab(j, block, gate_w.shape[1])
    for i, part in enumerate(
        (
            dot(tok[...], gate_w[:, cols]),
            dot(tok[...], up_w[:, cols]),
            dot(grad[...], down_w[...], NT),
        )
    ):
        mine[i] = part[:half]
        send[i] = part[half:]


def partial_sums(pick, pieces, gate_w, up_w, down_w):
    rows = pick.shape[0]
    half = rows // 2
    width, hidden = gate_w.shape
    block = block_of(hidden, 128, 512)
    part = jax.ShapeDtypeStruct((3, half, hidden), F32)
    full = jax.ShapeDtypeStruct((rows, width), BF)
    part_spec = pl.BlockSpec((3, half, block), lambda j: (0, 0, j))
    return pl.pallas_call(
        lambda *refs: sums_body(half, block, *refs),
        grid=(hidden // block,),
        out_shape=(part, part, full, full),
        in_specs=[VMEM, VMEM, VMEM, VMEM, pl.BlockSpec((block, width), lambda j: (j, 0))],
        out_specs=(part_spec, part_spec, pl.BlockSpec((rows, width), lambda j: (0, 0)), pl.BlockSpec((rows, width), lambda j: (0, 0))),
        compiler_params=params(16 << 20),
        cost_estimate=pl.CostEstimate(
            flops=6 * rows * width * hidden, transcendentals=0, bytes_accessed=2 * width * hidden
        ),
        name="sums",
    )(pick, pieces, gate_w, up_w, down_w)


def tokens_body(half, pick, grad, own, other, gate_w, up_w, total, down_grad, gate_g, up_g, all_h, gate_p, up_p):
    i = pl.program_id(0)

    @pl.when(i == 0)
    def _():
        all_h[:half] = own[0].astype(F32)
        all_h[half:] = other[0].astype(F32)
        for k, both, placed in ((1, gate_g, gate_p), (2, up_g, up_p)):
            rows = jnp.concatenate([own[k].astype(F32), other[k].astype(F32)], axis=0).astype(BF)
            both[...] = rows
            placed[...] = dot(pick[...], rows, TN).astype(BF)

    wide = total.shape[1]

    @pl.when(i < gate_w.shape[0] // wide)
    def _():
        rows = slab(i, wide, gate_w.shape[0])
        total[...] = dot(gate_p[...], gate_w[rows, :], NT) + dot(up_p[...], up_w[rows, :], NT)

    tall = down_grad.shape[0]

    @pl.when(i < all_h.shape[1] // tall)
    def _():
        cols = slab(i, tall, all_h.shape[1])
        down_grad[...] = dot(all_h[:, cols].astype(BF), grad[...], TN).astype(BF)


def token_grads(pick, grad, own, other, gate_w, up_w):
    rows, slots = pick.shape
    width, hidden = gate_w.shape
    half = rows // 2
    wide, tall = block_of(width, 128, 256), block_of(hidden, 128, 512)
    n_wide, n_tall = width // wide, hidden // tall
    both = jax.ShapeDtypeStruct((rows, hidden), BF)
    whole = pl.BlockSpec((rows, hidden), lambda i: (0, 0))
    return pl.pallas_call(
        lambda *refs: tokens_body(half, *refs),
        grid=(max(n_wide, n_tall),),
        out_shape=(
            jax.ShapeDtypeStruct((slots, width), F32),
            jax.ShapeDtypeStruct((hidden, width), BF),
            both,
            both,
        ),
        in_specs=[VMEM] * 6,
        out_specs=(
            pl.BlockSpec((slots, wide), lambda i: (0, jnp.minimum(i, n_wide - 1))),
            pl.BlockSpec((tall, width), lambda i: (jnp.minimum(i, n_tall - 1), 0)),
            whole,
            whole,
        ),
        scratch_shapes=[
            pltpu.VMEM((rows, hidden), F32),
            pltpu.VMEM((slots, hidden), BF),
            pltpu.VMEM((slots, hidden), BF),
        ],
        compiler_params=params(20 << 20),
        cost_estimate=pl.CostEstimate(
            flops=8 * rows * width * hidden, transcendentals=0, bytes_accessed=6 * width * hidden
        ),
        name="token_grads",
    )(pick, grad, own, other, gate_w, up_w)


def weights_body(tok, gate_g, up_g, gate_out, up_out):
    rows = tok[...].astype(BF)
    gate_out[...] = dot(rows, gate_g[...], TN).astype(BF)
    up_out[...] = dot(rows, up_g[...], TN).astype(BF)


def weight_grads(tok, gate_g, up_g):
    rows, width = tok.shape
    hidden = gate_g.shape[1]
    block = block_of(width, 128, 256)
    out = jax.ShapeDtypeStruct((width, hidden), BF)
    out_spec = pl.BlockSpec((block, hidden), lambda i: (i, 0))
    return pl.pallas_call(
        weights_body,
        grid=(width // block,),
        out_shape=(out, out),
        in_specs=[pl.BlockSpec((rows, block), lambda i: (0, i)), VMEM, VMEM],
        out_specs=(out_spec, out_spec),
        compiler_params=params(24 << 20),
        cost_estimate=pl.CostEstimate(
            flops=400 * rows * width * hidden, transcendentals=0, bytes_accessed=4 * width * hidden
        ),
        name="weight_grads",
    )(tok, gate_g, up_g)


def hidden_grads(sums):
    gate_sum, up_sum, back_sum = sums[0], sums[1], sums[2]
    sigmoid_gate = 1.0 / (1.0 + jnp.exp(-gate_sum))
    activated = gate_sum * sigmoid_gate
    hidden = (activated * up_sum).astype(BF)
    grad_up = (back_sum * activated).astype(BF)
    slope = sigmoid_gate * (1.0 + gate_sum * (1.0 - sigmoid_gate))
    grad_gate = (back_sum * up_sum * slope).astype(BF)
    return jnp.stack([hidden, grad_gate, grad_up])


def shards(n_row, n_col, tokens, grad_out, gate_w, up_w, down_w):
    here, width = tokens.shape
    slot = -(-here // 8) * 8
    count = here * n_col
    half = -(-count // 16) * 8
    me, col = lax.axis_index("row"), lax.axis_index("col")

    def shift(x, axis, n, s):
        return lax.ppermute(x, axis, [(i, (i + s) % n) for i in range(n)])

    piece = jnp.pad(jnp.stack([tokens, grad_out]), ((0, 0), (0, slot - here), (0, 0)))
    pieces = [piece] + [shift(piece, "col", n_col, s) for s in range(1, n_col)]
    gate_v, up_v = [pltpu.with_memory_space_constraint(w, pltpu.VMEM) for w in load(gate_w, up_w)]
    pieces = jnp.stack(pieces, axis=1).reshape(2, n_col * slot, width)

    k = lax.iota(jnp.int32, n_col * slot)
    source = (col - k // slot) % n_col
    token = jnp.where(k % slot < here, source * here + k % slot, -1)
    side = jnp.where(token < half, 0, 1)
    row = jnp.where(token < 0, -1, (side ^ (me % 2)) * half + token - side * half)
    pick = (lax.iota(jnp.int32, 2 * half)[:, None] == row[None, :]).astype(BF)

    mine, send, tok, grad = partial_sums(pick, pieces, gate_v, up_v, down_w)

    partner = [(i, i ^ 1) for i in range(n_row)]
    part = mine + lax.ppermute(send, "row", partner)
    out = part.astype(BF)
    total = part
    for s in range(2, n_row, 2):
        total = total + lax.ppermute(out, "row", [(i, (i + s) % n_row) for i in range(n_row)]).astype(F32)
    own = hidden_grads(total)
    other = lax.ppermute(own, "row", partner)

    token_part, down_grad, gate_g, up_g = token_grads(pick, grad, own, other, gate_v, up_v)
    token_part = token_part.reshape(n_col, slot, width)
    token_grad = token_part[0, :here]
    for s in range(1, n_col):
        token_grad = token_grad + shift(token_part[s], "col", n_col, n_col - s)[:here]
    gate_grad, up_grad = weight_grads(tok, gate_g, up_g)
    return (token_grad.astype(BF), gate_grad, up_grad, down_grad)


def solution(mesh):
    n_row, n_col = mesh.shape["row"], mesh.shape["col"]
    placed = (P("col", "row"), P("col", "row"), P("row", "col"), P("row", "col"), P("col", "row"))
    return jax.shard_map(
        lambda *args: shards(n_row, n_col, *args),
        mesh=mesh,
        in_specs=placed,
        out_specs=(P("col", "row"), P("row", "col"), P("row", "col"), P("col", "row")),
        check_vma=False,
    )
```
